32 devices in a mesh: groups: 2 (over y), seq: 4 (over z), head: 2 (over x), rep: 2 (over core).
Axes of the slice: x: 2, y: 2, z: 4, core: 2. Of those that a mesh axis runs over, the one named last changes fastest.
Arguments:
- kv_cache: bfloat16 [2, 256, 8, 128, 256], P(None, ('groups', 'seq'), 'head', 'rep'), parts along dimension 1, may hold values from -6 to 6
- keep_list: int32 [4, 64], P('groups'), parts along dimension 0, may hold values from -1 to 127, as said below
- page_slot: int32 [4, 64], P('groups'), parts along dimension 0, may hold values from -1 to 63, as said below
Outputs:
- paged_cache: bfloat16 [2, 128, 8, 128, 256], P(None, ('groups', 'seq'), 'head', 'rep'), parts along dimension 1
- page_bounds: bfloat16 [2, 128, 8, 2, 128], P(None, ('groups', 'seq'), 'head'), parts along dimension 1
The draws below stay inside these ranges and needn't reach their ends.
There are 2 independent parts, one for each index of `groups`. The reference program is written for one: setup_inputs(seed, part) draws one part's arguments, and reference() takes and returns one part's arrays. A program takes and returns all parts, laid end to end along the dimension named above; each array names one. Nothing has to cross between parts.
Inputs may be any that keep to these rules, and one draw needn't show every extreme that they name: `keep_list`: row l holds count_l distinct block indices in rising order, then -1 in the remaining entries. Of one row, at most 16 listed blocks lie on one seq shard (blocks s * 32 to s * 32 + 31); row 0 reaches this on every shard. `page_slot`: entry (l, j) is the page of block keep_list[l, j]: distinct pages for the count_l listed blocks of a row, -1 after them. Of one row, at most 5 blocks of one seq shard go to pages of one owner (pages o * 16 to o * 16 + 15), and this is reached in every draw.
All inputs are finite; a program needn't handle non-finite values.
Results may differ from the reference program's by a relative error of at most 0.001.
Values may be sent and summed in bfloat16 or wider, within the bound.
A program may use at most 64 MiB of HBM per device.

```python
import jax
import jax.numpy as jnp

KVH = 8
HD = 128
BLK = 128
LAYERS = 2
BLK_DEV = 32
BLOCKS = 128


def draw_plan(key):
    page_dev = BLK_DEV // 2
    seq_count = BLOCKS // BLK_DEV
    page_total = page_dev * seq_count
    keep_rows = []
    slot_rows = []
    for layer in range(LAYERS):
        layer_key = jax.random.fold_in(key, 7000 + layer)
        shift_key, local_key, used_key = jax.random.split(layer_key, 3)
        shuffled = jax.random.permutation(shift_key, seq_count).astype(jnp.int32)
        page_index = jnp.arange(page_dev, dtype=jnp.int32)
        shift_value = shuffled[jnp.maximum(page_index - 1, 0) % seq_count]
        owner_index = jnp.arange(seq_count, dtype=jnp.int32)
        source = (owner_index[:, None] + shift_value[None, :]) % seq_count
        scores = jax.random.randint(local_key, (seq_count, BLK_DEV), 0, 2 ** 20) * BLK_DEV + jnp.arange(BLK_DEV, dtype=jnp.int32)[None, :]
        local_order = jnp.argsort(scores, axis=1).astype(jnp.int32)
        local_block = local_order[source, jnp.broadcast_to(page_index[None, :], source.shape)]
        block_id = (source * BLK_DEV + local_block).reshape(-1).astype(jnp.int32)
        keep_count = page_total - layer * page_total // (2 * LAYERS)
        used = jax.random.permutation(used_key, page_total).astype(jnp.int32)[:keep_count]
        kept_blocks = block_id[used]
        sorter = jnp.argsort(kept_blocks)
        padding = jnp.full((page_total - keep_count,), -1, jnp.int32)
        keep_rows.append(jnp.concatenate([kept_blocks[sorter], padding]))
        slot_rows.append(jnp.concatenate([used[sorter], padding]))
    return (jnp.stack(keep_rows, axis=0).astype(jnp.int32), jnp.stack(slot_rows, axis=0).astype(jnp.int32))


def draw_keep_list(key, part):
    return draw_plan(key)[0]


def draw_page_slot(key, part):
    return draw_plan(key)[1]


def block_levels(rng, extent, pieces, least, largest):
    gain, own = 1.0, jax.random.fold_in(rng, 6)
    for position, parts in pieces:
        draws = jnp.exp(jax.random.uniform(jax.random.fold_in(own, position), (parts,), jnp.float32, least / len(pieces), largest / len(pieces)))
        gain = gain * jnp.repeat(draws, extent[position] // parts).reshape([-1 if axis == position else 1 for axis in range(len(extent))])
    return gain


def scatter_about(stream_key, dims, width, limit, cuts=(), held_as=jnp.bfloat16):
    factor_of = block_levels(stream_key, dims, cuts, -0.22, 0.18) if cuts else 1.0
    result = jax.random.normal(stream_key, dims, jnp.float32) * width * factor_of
    return jnp.minimum(jnp.maximum(result, -limit), limit).astype(held_as)


def setup_inputs(seed: int = 0, part: int = 0) -> dict:
    keys = jax.random.split(jax.random.key(seed), 4)
    part_splits = jax.random.split(jax.random.fold_in(keys[3], part), 4)
    kv_cache = scatter_about(part_splits[0], (LAYERS, BLOCKS, KVH, BLK, 2 * HD), 1.0, 6.0, ((1, 4), (2, 2), (3, 2)))
    keep_list = draw_keep_list(jax.random.fold_in(jax.random.fold_in(keys[3], part), 71), part)
    page_slot = draw_page_slot(jax.random.fold_in(jax.random.fold_in(keys[3], part), 71), part)
    return dict(kv_cache=kv_cache, keep_list=keep_list, page_slot=page_slot)


def reference(kv_cache, keep_list, page_slot):
    layer_count, page_count = keep_list.shape
    layer_pages = []
    for layer in range(layer_count):
        keep_count = page_count - (layer * page_count) // (2 * layer_count)
        kept_blocks = keep_list[layer, :keep_count].astype(jnp.int32)
        slot_list = page_slot[layer, :keep_count].astype(jnp.int32)
        chosen = kv_cache[layer][kept_blocks]
        empty_pages = jnp.zeros((page_count,) + kv_cache.shape[2:], kv_cache.dtype)
        layer_pages.append(empty_pages.at[slot_list].set(chosen))
    paged_cache = jnp.stack(layer_pages, axis=0)
    key_part = paged_cache[..., :HD]
    page_bounds = jnp.stack([jnp.max(key_part, axis=3), jnp.min(key_part, axis=3)], axis=3)
    return paged_cache, page_bounds
```

```python
import functools

import jax
import jax.numpy as jnp
from jax import lax
from jax.experimental import pallas as pl
from jax.experimental.pallas import tpu as pltpu
from jax.sharding import PartitionSpec as P

MESH = pl.DeviceIdType.MESH
ANY = pl.BlockSpec(memory_space=pl.ANY)
SMEM = pl.BlockSpec(memory_space=pltpu.SMEM)
VMEM = pl.BlockSpec(memory_space=pltpu.VMEM)

SHARED = (2, 3, 4, 5)


def combined_all(part, axis, combine):
    gathered = jax.tree.map(lambda a: lax.all_gather(a, axis), part)

    def take(source):
        return jax.tree.map(lambda a: lax.dynamic_index_in_dim(a, source, 0, False), gathered)

    return lax.fori_loop(
        1, lax.axis_size(axis), lambda source, state: combine(state, take(source)), take(0)
    )


def pack_slots(block_rows, sent_here, destination, local_block, slot_width):
    blk_dev = block_rows.shape[1]
    slot_hot = (
        destination[:, :, None] == jnp.arange(slot_width, dtype=jnp.int32)[None, None, :]
    ) & sent_here[:, :, None]
    block_hot = local_block[:, :, None] == jnp.arange(blk_dev, dtype=jnp.int32)[None, None, :]
    select = jnp.einsum(
        "ljw,ljb->lwb", slot_hot.astype(jnp.float32), block_hot.astype(jnp.float32)
    ).astype(jnp.bfloat16)
    return jnp.einsum(
        "lwb,lbr->lwr", select, block_rows, preferred_element_type=jnp.float32
    ).astype(jnp.bfloat16)


def place_index(takers, in_page, incoming, page_dev):
    page_hot = (
        in_page[:, :, None] == jnp.arange(page_dev, dtype=jnp.int32)[None, None, :]
    ) & takers[:, :, None]
    return jnp.sum(jnp.where(page_hot, incoming[:, :, None] + 1, 0), axis=1) - 1


def place_pages(target, shard_part):
    width = shard_part.shape[1]
    one_hot = (target[:, :, None] == jnp.arange(width, dtype=jnp.int32)[None, None, :]).astype(
        jnp.bfloat16
    )
    return jnp.einsum("lpn,lnr->lpr", one_hot, shard_part, preferred_element_type=jnp.float32)


def extend(first, second):
    return (jnp.maximum(first[0], second[0]), jnp.minimum(first[1], second[1]))


def any_line(kv_cache, keep_list, page_slot):
    layer_count, page_count = keep_list.shape
    blk_dev = kv_cache.shape[1]
    seq_count = lax.axis_size("seq")
    page_dev = page_count // seq_count
    capacity = (page_dev - 2) // seq_count + 2
    seq_index = lax.axis_index("seq")
    block_rows = kv_cache.reshape(layer_count, blk_dev, -1)
    position = jnp.arange(page_count, dtype=jnp.int32)
    counts = jnp.array(
        [page_count - layer * page_count // (2 * layer_count) for layer in range(layer_count)],
        jnp.int32,
    )
    listed = position[None, :] < counts[:, None]
    source = keep_list // blk_dev
    local_block = keep_list % blk_dev
    owner_index = page_slot // page_dev
    in_page = page_slot % page_dev
    earlier = (position[None, None, :] < position[None, :, None]) & listed[:, None, :]
    same_source = source[:, :, None] == source[:, None, :]
    sent_here = listed & (source == seq_index)
    takers = listed & (owner_index == seq_index)
    same_owner = owner_index[:, :, None] == owner_index[:, None, :]
    slot_rank = jnp.sum(earlier & same_source & same_owner, axis=2)
    packed = pack_slots(
        block_rows, sent_here, owner_index * capacity + slot_rank, local_block, seq_count * capacity
    )
    received = lax.all_to_all(packed, "seq", split_axis=1, concat_axis=1, tiled=True)
    target = place_index(takers, in_page, source * capacity + slot_rank, page_dev)
    gathered = place_pages(target, received)
    paged_cache = gathered.astype(jnp.bfloat16).reshape(
        (layer_count, page_dev) + kv_cache.shape[2:]
    )
    head_width = kv_cache.shape[-1] // 2
    key_part = paged_cache[..., :head_width]
    key_high = jnp.max(key_part, axis=3)
    key_low = jnp.min(key_part, axis=3)
    upper_bound, lower_bound = combined_all((key_high, key_low), "rep", extend)
    page_bounds = jnp.stack([upper_bound, lower_bound], axis=3)
    return (paged_cache, page_bounds)


def pack_kernel(table, blocks, packed, held, read_sem, write_sem):
    count = packed.shape[0]

    def read(k):
        return pltpu.make_async_copy(blocks.at[table[k]], held.at[k], read_sem.at[k])

    def write(k):
        return pltpu.make_async_copy(held.at[k], packed.at[k], write_sem.at[k])

    @pl.loop(0, count)
    def _(k):
        read(k).start()

    @pl.loop(0, count)
    def _(k):
        read(k).wait()
        write(k).start()

    @pl.loop(0, count)
    def _(k):
        write(k).wait()


def place_kernel(table, slots, bounds, pages, page_bounds, held, read_sem, write_sem):
    count = pages.shape[0]

    def read(k):
        return pltpu.make_async_copy(slots.at[table[k]], held.at[k], read_sem.at[k])

    def write(k):
        return pltpu.make_async_copy(held.at[k], pages.at[k], write_sem.at[k])

    @pl.loop(0, count)
    def _(k):
        read(k).start()

    @pl.loop(0, count)
    def _(k):
        page_bounds[k] = bounds[table[k]]

    @pl.loop(0, count)
    def _(k):
        read(k).wait()
        write(k).start()

    @pl.loop(0, count)
    def _(k):
        write(k).wait()


def exchange_kernel(
    cap, shared, packed, slots, bounds,
    held, mine, theirs, send_sem, recv_sem, relay_sem, local_sem, write_sem, rep_send, rep_recv,
):
    me = lax.axis_index("seq")
    half, lane = me // 2, me % 2
    partner = me + 1 - 2 * lane
    near, far = 2 - half, 3 - 3 * half
    inner = half + lane == 1
    other = 1 - lax.axis_index("rep")
    alone = cap - shared
    heads, width = held.shape[1], mine.shape[2]

    barrier = pltpu.get_barrier_semaphore()
    for step in range(1, 4):
        pl.semaphore_signal(
            barrier, inc=1, device_id={"seq": (me + step) % 4}, device_id_type=MESH
        )
    pl.semaphore_signal(barrier, inc=1, device_id={"rep": other}, device_id_type=MESH)
    pl.semaphore_wait(barrier, 4)

    def remote(source, place, target, sem):
        return pltpu.make_async_remote_copy(
            src_ref=source,
            dst_ref=held.at[place],
            send_sem=sem,
            recv_sem=recv_sem.at[place],
            device_id={"seq": target},
            device_id_type=MESH,
        )

    def to_near(q):
        return remote(packed.at[q], lane * cap + q, near, send_sem.at[q])

    def to_far(q):
        return remote(packed.at[q + alone], lane * cap + q, far, send_sem.at[q + alone])

    def to_partner(q):
        return remote(packed.at[2 * cap + q], 2 * cap + q, partner, send_sem.at[2 * cap + q])

    def relay(place, sem):
        return remote(held.at[place], place, partner, relay_sem.at[sem])

    def landed(place):
        pltpu.make_async_copy(held.at[place], held.at[place], recv_sem.at[place]).wait()

    def own(q):
        return pltpu.make_async_copy(
            packed.at[3 * cap + q], held.at[3 * cap + q], local_sem.at[q]
        )

    def write(place):
        return pltpu.make_async_copy(held.at[place], slots.at[place], write_sem.at[place])

    def finish(place):
        keys = held[place, :, :, :width].astype(jnp.float32)
        mine[place, :heads] = jnp.max(keys, axis=1)
        mine[place, heads:] = jnp.min(keys, axis=1)
        write(place).start()

    def swap(start, count, k):
        return pltpu.make_async_remote_copy(
            src_ref=mine.at[pl.ds(start, count)],
            dst_ref=theirs.at[pl.ds(start, count)],
            send_sem=rep_send.at[k],
            recv_sem=rep_recv.at[k],
            device_id={"rep": other},
            device_id_type=MESH,
        )

    def join(start, count):
        @pl.loop(0, count)
        def _(q):
            a, b = mine[start + q], theirs[start + q]
            bounds[start + q, :heads] = jnp.maximum(a[:heads], b[:heads])
            bounds[start + q, heads:] = jnp.minimum(a[heads:], b[heads:])

    @pl.when(jnp.logical_not(inner))
    def _():
        @pl.loop(0, cap)
        def _(q):
            to_partner(q).start()

    @pl.loop(0, shared)
    def _(q):
        to_near(q).start()

    @pl.loop(shared, cap)
    def _(q):
        to_far(q).start()
        to_near(q).start()

    @pl.when(inner)
    def _():
        @pl.loop(0, cap)
        def _(q):
            to_partner(q).start()

    @pl.loop(0, cap)
    def _(q):
        own(q).start()

    empty = 4 * cap
    held[empty] = jnp.zeros(held.shape[1:], held.dtype)
    bounds[empty] = jnp.zeros(bounds.shape[1:], bounds.dtype)

    @pl.loop(0, cap)
    def _(q):
        own(q).wait()
        finish(3 * cap + q)

    write(empty).start()
    first, second = half * cap, (1 - half) * cap

    if shared:
        @pl.when(inner)
        def _():
            @pl.loop(0, shared)
            def _(q):
                landed(first + q)
                relay(first + q, q).start()

            @pl.loop(0, shared)
            def _(q):
                landed(second + q)
                relay(second + q, shared + q).start()

    @pl.loop(0, cap)
    def _(q):
        landed(2 * cap + q)
        finish(2 * cap + q)

    swap(2 * cap, 2 * cap, 0).start()

    def collect(start):
        if shared:
            @pl.when(jnp.logical_not(inner))
            def _():
                @pl.loop(0, shared)
                def _(q):
                    landed(start + q)

            @pl.loop(0, shared)
            def _(q):
                finish(start + q)

        @pl.loop(shared, cap)
        def _(q):
            landed(start + q)
            finish(start + q)

    collect(first)
    swap(2 * cap, 2 * cap, 0).wait()
    join(2 * cap, 2 * cap)
    swap(first, cap, 1).start()
    collect(second)

    @pl.loop(2 * cap, 4 * cap + 1)
    def _(k):
        write(k).wait()

    @pl.loop(0, cap)
    def _(q):
        write(first + q).wait()

    swap(second, cap, 2).start()
    swap(first, cap, 1).wait()
    join(first, cap)

    @pl.loop(0, 2 * cap - shared)
    def _(q):
        to_near(q).wait_send()

    @pl.loop(0, cap)
    def _(q):
        to_partner(q).wait_send()
        write(second + q).wait()

    if shared:
        @pl.when(inner)
        def _():
            @pl.loop(0, shared)
            def _(q):
                relay(first + q, q).wait_send()
                relay(second + q, shared + q).wait_send()

    swap(second, cap, 2).wait()
    join(second, cap)


def exchange(cap, shared, collective, packed, heads, width):
    page = packed.shape[1:]
    count = 4 * cap + 1
    dma = pltpu.SemaphoreType.DMA
    return pl.pallas_call(
        functools.partial(exchange_kernel, cap, shared),
        out_shape=(
            jax.ShapeDtypeStruct((count,) + page, packed.dtype),
            jax.ShapeDtypeStruct((count, 2 * heads, width), jnp.float32),
        ),
        in_specs=[ANY],
        out_specs=(ANY, VMEM),
        scratch_shapes=[
            pltpu.VMEM((count,) + page, packed.dtype),
            pltpu.VMEM((4 * cap, 2 * heads, width), jnp.float32),
            pltpu.VMEM((4 * cap, 2 * heads, width), jnp.float32),
            dma((3 * cap,)),
            dma((3 * cap,)),
            dma((max(2 * shared, 1),)),
            dma((cap,)),
            dma((count,)),
            dma((3,)),
            dma((3,)),
        ],
        compiler_params=pltpu.CompilerParams(collective_id=collective, has_side_effects=True),
    )(packed)


def line_of_four(kv_cache, keep_list, page_slot):
    layers, page_count = keep_list.shape
    blk_dev = kv_cache.shape[1]
    page = kv_cache.shape[2:]
    heads, width = page[0], page[-1] // 2
    page_dev = page_count // 4
    cap = layers * ((page_dev - 2) // 4 + 2)
    dma = pltpu.SemaphoreType.DMA
    me = lax.axis_index("seq")

    position = jnp.arange(page_count, dtype=jnp.int32)
    counts = jnp.array(
        [page_count - layer * page_count // (2 * layers) for layer in range(layers)], jnp.int32
    )
    listed = (position[None, :] < counts[:, None]).reshape(-1)
    layer = jnp.repeat(jnp.arange(layers, dtype=jnp.int32), page_count)
    keep = jnp.where(listed, keep_list.reshape(-1), 0)
    slot = jnp.where(listed, page_slot.reshape(-1), 0)
    source, owner = keep // blk_dev, slot // page_dev
    pair = jnp.where(listed, source * 4 + owner, -1)
    place = jnp.arange(layers * page_count, dtype=jnp.int32)
    rank = jnp.sum(
        (pair[:, None] == pair[None, :]) & (place[None, :] < place[:, None]), axis=1
    ).astype(jnp.int32)
    crossing = listed & (source // 2 != owner // 2)
    pools = jnp.sum(
        crossing[None, :] & (source[None, :] == jnp.arange(4, dtype=jnp.int32)[:, None]), axis=1
    )
    largest = jnp.max(pools).astype(jnp.int32).reshape(1)
    if lax.axis_size("groups") > 1:
        size = lax.axis_size("groups")
        told = largest
        for step in range(1, size):
            passed = lax.ppermute(told, "groups", [(i, (i + step) % size) for i in range(size)])
            largest = jnp.maximum(largest, passed)
    sizes = [s for s in SHARED if s <= cap]
    fits = sum((largest[0] <= 2 * cap - s).astype(jnp.int32) for s in sizes)
    shared = jnp.array([0] + sizes, jnp.int32)[fits]
    alone = cap - shared

    to_far = crossing & ((owner == 0) | (owner == 3))
    spill = rank - alone
    lone = rank < alone
    in_region = jnp.where(
        crossing,
        jnp.where(lone, shared + rank, jnp.where(to_far, shared - 1 - spill, spill)),
        rank,
    )
    sent = jnp.where(
        crossing,
        in_region + jnp.where(to_far & lone, alone, 0),
        in_region + jnp.where(source == owner, 3 * cap, 2 * cap),
    )
    got = in_region + jnp.where(
        crossing, (source % 2) * cap, jnp.where(source == owner, 3 * cap, 2 * cap)
    )
    spots = jnp.arange(4 * cap, dtype=jnp.int32)
    from_me = listed & (source == me)
    pack_table = jnp.sum(
        jnp.where(
            from_me[None, :] & (sent[None, :] == spots[:, None]),
            (layer * blk_dev + keep % blk_dev)[None, :],
            0,
        ),
        axis=1,
    ).astype(jnp.int32)
    pages = jnp.arange(layers * page_dev, dtype=jnp.int32)
    to_me = listed & (owner == me)
    place_table = 4 * cap + jnp.sum(
        jnp.where(
            to_me[None, :] & ((layer * page_dev + slot % page_dev)[None, :] == pages[:, None]),
            (got - 4 * cap)[None, :],
            0,
        ),
        axis=1,
    ).astype(jnp.int32)

    packed = pl.pallas_call(
        pack_kernel,
        out_shape=jax.ShapeDtypeStruct((4 * cap,) + page, kv_cache.dtype),
        in_specs=[SMEM, ANY],
        out_specs=ANY,
        scratch_shapes=[
            pltpu.VMEM((4 * cap,) + page, kv_cache.dtype),
            dma((4 * cap,)),
            dma((4 * cap,)),
        ],
    )(pack_table, kv_cache.reshape((layers * blk_dev,) + page))

    slots, bounds = lax.switch(
        fits,
        [
            functools.partial(exchange, cap, s, k, heads=heads, width=width)
            for k, s in enumerate([0] + sizes)
        ],
        packed,
    )

    paged, page_bounds = pl.pallas_call(
        place_kernel,
        out_shape=(
            jax.ShapeDtypeStruct((layers * page_dev,) + page, kv_cache.dtype),
            jax.ShapeDtypeStruct((layers * page_dev, 2 * heads, width), jnp.float32),
        ),
        in_specs=[SMEM, ANY, VMEM],
        out_specs=(ANY, VMEM),
        scratch_shapes=[
            pltpu.VMEM((layers * page_dev,) + page, kv_cache.dtype),
            dma((layers * page_dev,)),
            dma((layers * page_dev,)),
        ],
    )(place_table, slots, bounds)
    page_bounds = page_bounds.reshape(layers, page_dev, 2, heads, width)
    return (
        paged.reshape((layers, page_dev) + page),
        page_bounds.transpose(0, 1, 3, 2, 4).astype(kv_cache.dtype),
    )


def on_device(kv_cache, keep_list, page_slot):
    body = line_of_four if lax.axis_size("seq") == 4 else any_line
    return body(kv_cache, keep_list, page_slot)


def solution(mesh):
    in_specs = (
        P(None, ("groups", "seq"), "head", "rep", None),
        P("groups", None),
        P("groups", None),
    )
    out_specs = (
        P(None, ("groups", "seq"), "head", "rep", None),
        P(None, ("groups", "seq"), "head", None, None),
    )
    return jax.shard_map(
        on_device, mesh=mesh, in_specs=in_specs, out_specs=out_specs, check_vma=False
    )
```

```python
import functools

import jax
import jax.numpy as jnp
from jax import lax
from jax.experimental import pallas as pl
from jax.experimental.pallas import tpu as pltpu
from jax.sharding import PartitionSpec as P

MESH = pl.DeviceIdType.MESH
HBM = pl.BlockSpec(memory_space=pltpu.HBM)
SMEM = pl.BlockSpec(memory_space=pltpu.SMEM)
GRANT = 8 << 20
PACK_GRANT = 54 << 20
VMEM = pl.BlockSpec(memory_space=pltpu.VMEM)


def combined_all(part, axis, combine):
    gathered = jax.tree.map(lambda a: lax.all_gather(a, axis), part)

    def take(source):
        return jax.tree.map(lambda a: lax.dynamic_index_in_dim(a, source, 0, False), gathered)

    return lax.fori_loop(
        1, lax.axis_size(axis), lambda source, state: combine(state, take(source)), take(0)
    )


def pack_slots(block_rows, sent_here, destination, local_block, slot_width):
    blk_dev = block_rows.shape[1]
    slot_hot = (
        destination[:, :, None] == jnp.arange(slot_width, dtype=jnp.int32)[None, None, :]
    ) & sent_here[:, :, None]
    block_hot = local_block[:, :, None] == jnp.arange(blk_dev, dtype=jnp.int32)[None, None, :]
    select = jnp.einsum(
        "ljw,ljb->lwb", slot_hot.astype(jnp.float32), block_hot.astype(jnp.float32)
    ).astype(jnp.bfloat16)
    return jnp.einsum(
        "lwb,lbr->lwr", select, block_rows, preferred_element_type=jnp.float32
    ).astype(jnp.bfloat16)


def place_index(takers, in_page, incoming, page_dev):
    page_hot = (
        in_page[:, :, None] == jnp.arange(page_dev, dtype=jnp.int32)[None, None, :]
    ) & takers[:, :, None]
    return jnp.sum(jnp.where(page_hot, incoming[:, :, None] + 1, 0), axis=1) - 1


def place_pages(target, shard_part):
    width = shard_part.shape[1]
    one_hot = (target[:, :, None] == jnp.arange(width, dtype=jnp.int32)[None, None, :]).astype(
        jnp.bfloat16
    )
    return jnp.einsum("lpn,lnr->lpr", one_hot, shard_part, preferred_element_type=jnp.float32)


def extend(first, second):
    return (jnp.maximum(first[0], second[0]), jnp.minimum(first[1], second[1]))


def any_line(kv_cache, keep_list, page_slot):
    layer_count, page_count = keep_list.shape
    blk_dev = kv_cache.shape[1]
    seq_count = lax.axis_size("seq")
    page_dev = page_count // seq_count
    capacity = (page_dev - 2) // seq_count + 2
    seq_index = lax.axis_index("seq")
    block_rows = kv_cache.reshape(layer_count, blk_dev, -1)
    position = jnp.arange(page_count, dtype=jnp.int32)
    counts = jnp.array(
        [page_count - layer * page_count // (2 * layer_count) for layer in range(layer_count)],
        jnp.int32,
    )
    listed = position[None, :] < counts[:, None]
    source = keep_list // blk_dev
    local_block = keep_list % blk_dev
    owner_index = page_slot // page_dev
    in_page = page_slot % page_dev
    earlier = (position[None, None, :] < position[None, :, None]) & listed[:, None, :]
    same_source = source[:, :, None] == source[:, None, :]
    sent_here = listed & (source == seq_index)
    takers = listed & (owner_index == seq_index)
    same_owner = owner_index[:, :, None] == owner_index[:, None, :]
    slot_rank = jnp.sum(earlier & same_source & same_owner, axis=2)
    packed = pack_slots(
        block_rows, sent_here, owner_index * capacity + slot_rank, local_block, seq_count * capacity
    )
    received = lax.all_to_all(packed, "seq", split_axis=1, concat_axis=1, tiled=True)
    target = place_index(takers, in_page, source * capacity + slot_rank, page_dev)
    gathered = place_pages(target, received)
    paged_cache = gathered.astype(jnp.bfloat16).reshape(
        (layer_count, page_dev) + kv_cache.shape[2:]
    )
    head_width = kv_cache.shape[-1] // 2
    key_part = paged_cache[..., :head_width]
    key_high = jnp.max(key_part, axis=3)
    key_low = jnp.min(key_part, axis=3)
    upper_bound, lower_bound = combined_all((key_high, key_low), "rep", extend)
    page_bounds = jnp.stack([upper_bound, lower_bound], axis=3)
    return (paged_cache, page_bounds)


def pack_kernel(table, blocks, packed, read_sem):
    count = packed.shape[0]

    def read(k):
        return pltpu.make_async_copy(blocks.at[table[k]], packed.at[k], read_sem.at[k])

    @pl.loop(0, count)
    def _(k):
        read(k).start()

    @pl.loop(0, count)
    def _(k):
        read(k).wait()


def place_kernel(table, slots, bounds, pages, page_bounds, write_sem):
    count, heads = page_bounds.shape[0], page_bounds.shape[1]

    def write(k):
        return pltpu.make_async_copy(slots.at[table[k]], pages.at[k], write_sem.at[k])

    @pl.loop(0, count)
    def _(k):
        write(k).start()

    @pl.loop(0, count)
    def _(k):
        both = bounds[table[k]]
        page_bounds[k] = jnp.stack([both[:heads], both[heads:]], axis=1).astype(page_bounds.dtype)

    @pl.loop(0, count)
    def _(k):
        write(k).wait()


def exchange_kernel(
    cap, shared, packed, held, bounds,
    mine, theirs, send_sem, recv_sem, relay_sem, rep_send, rep_recv,
):
    me = lax.axis_index("seq")
    half, lane = me // 2, me % 2
    partner = me + 1 - 2 * lane
    near, far = 2 - half, 3 - 3 * half
    inner = half + lane == 1
    other = 1 - lax.axis_index("rep")
    alone = cap - shared
    heads, width = held.shape[1], mine.shape[2]

    barrier = pltpu.get_barrier_semaphore()
    for step in range(1, 4):
        pl.semaphore_signal(
            barrier, inc=1, device_id={"seq": (me + step) % 4}, device_id_type=MESH
        )
    pl.semaphore_signal(barrier, inc=1, device_id={"rep": other}, device_id_type=MESH)
    pl.semaphore_wait(barrier, 4)

    def remote(source, place, target, sem):
        return pltpu.make_async_remote_copy(
            src_ref=source,
            dst_ref=held.at[place],
            send_sem=sem,
            recv_sem=recv_sem.at[place],
            device_id={"seq": target},
            device_id_type=MESH,
        )

    def to_near(q):
        return remote(packed.at[q], lane * cap + q, near, send_sem.at[q])

    def to_far(q):
        return remote(packed.at[q + alone], lane * cap + q, far, send_sem.at[q + alone])

    def to_partner(q):
        return remote(packed.at[2 * cap + q], 2 * cap + q, partner, send_sem.at[2 * cap + q])

    def relay(place, sem):
        return remote(held.at[place], place, partner, relay_sem.at[sem])

    def landed(place):
        pltpu.make_async_copy(held.at[place], held.at[place], recv_sem.at[place]).wait()

    def finish(place):
        extremes(place, held[place, :, :, :width])

    def extremes(place, keys):
        keys = keys.astype(jnp.float32)
        mine[place, :heads] = jnp.max(keys, axis=1)
        mine[place, heads:] = jnp.min(keys, axis=1)

    def swap(start, count, k):
        return pltpu.make_async_remote_copy(
            src_ref=mine.at[pl.ds(start, count)],
            dst_ref=theirs.at[pl.ds(start, count)],
            send_sem=rep_send.at[k],
            recv_sem=rep_recv.at[k],
            device_id={"rep": other},
            device_id_type=MESH,
        )

    def join(start, count):
        @pl.loop(0, count)
        def _(q):
            a, b = mine[start + q], theirs[start + q]
            bounds[start + q, :heads] = jnp.maximum(a[:heads], b[:heads])
            bounds[start + q, heads:] = jnp.minimum(a[heads:], b[heads:])

    @pl.when(jnp.logical_not(inner))
    def _():
        @pl.loop(0, cap)
        def _(q):
            to_partner(q).start()

    @pl.loop(0, shared)
    def _(q):
        to_near(q).start()

    @pl.loop(shared, cap)
    def _(q):
        to_far(q).start()
        to_near(q).start()

    @pl.when(inner)
    def _():
        @pl.loop(0, cap)
        def _(q):
            to_partner(q).start()

    empty = 4 * cap
    held[empty] = jnp.zeros(held.shape[1:], held.dtype)
    bounds[empty] = jnp.zeros(bounds.shape[1:], bounds.dtype)

    @pl.loop(0, cap)
    def _(q):
        block = packed[3 * cap + q]
        held[3 * cap + q] = block
        extremes(3 * cap + q, block[:, :, :width])

    first, second = half * cap, (1 - half) * cap

    if shared:
        @pl.when(inner)
        def _():
            @pl.loop(0, shared)
            def _(q):
                landed(first + q)
                relay(first + q, q).start()

            @pl.loop(0, shared)
            def _(q):
                landed(second + q)
                relay(second + q, shared + q).start()

    @pl.loop(0, cap)
    def _(q):
        landed(2 * cap + q)
        finish(2 * cap + q)

    swap(2 * cap, 2 * cap, 0).start()

    def collect(start):
        if shared:
            @pl.when(jnp.logical_not(inner))
            def _():
                @pl.loop(0, shared)
                def _(q):
                    landed(start + q)

            @pl.loop(0, shared)
            def _(q):
                finish(start + q)

        @pl.loop(shared, cap)
        def _(q):
            landed(start + q)
            finish(start + q)

    collect(first)
    swap(2 * cap, 2 * cap, 0).wait()
    join(2 * cap, 2 * cap)
    swap(first, cap, 1).start()
    collect(second)

    swap(first, cap, 1).wait()
    join(first, cap)
    swap(second, cap, 2).start()

    @pl.loop(0, 2 * cap - shared)
    def _(q):
        to_near(q).wait_send()

    @pl.loop(0, cap)
    def _(q):
        to_partner(q).wait_send()

    if shared:
        @pl.when(inner)
        def _():
            @pl.loop(0, shared)
            def _(q):
                relay(first + q, q).wait_send()
                relay(second + q, shared + q).wait_send()

    swap(second, cap, 2).wait()
    join(second, cap)


def exchange(cap, shared, collective, packed, heads, width):
    page = packed.shape[1:]
    count = 4 * cap + 1
    dma = pltpu.SemaphoreType.DMA
    return pl.pallas_call(
        functools.partial(exchange_kernel, cap, shared),
        out_shape=(
            pltpu.VMEM((count,) + page, packed.dtype),
            pltpu.VMEM((count, 2 * heads, width), jnp.float32),
        ),
        in_specs=[VMEM],
        out_specs=(VMEM, VMEM),
        scratch_shapes=[
            pltpu.VMEM((4 * cap, 2 * heads, width), jnp.float32),
            pltpu.VMEM((4 * cap, 2 * heads, width), jnp.float32),
            dma((3 * cap,)),
            dma((3 * cap,)),
            dma((max(2 * shared, 1),)),
            dma((3,)),
            dma((3,)),
        ],
        compiler_params=pltpu.CompilerParams(
            collective_id=collective, has_side_effects=True, vmem_limit_bytes=GRANT
        ),
    )(packed)


def line_of_four(kv_cache, keep_list, page_slot):
    layers, page_count = keep_list.shape
    blk_dev = kv_cache.shape[1]
    page = kv_cache.shape[2:]
    heads, width = page[0], page[-1] // 2
    page_dev = page_count // 4
    cap = layers * ((page_dev - 2) // 4 + 2)
    dma = pltpu.SemaphoreType.DMA
    me = lax.axis_index("seq")

    shape = (layers, page_count)
    layer = lax.broadcasted_iota(jnp.int32, shape, 0)
    position = lax.broadcasted_iota(jnp.int32, shape, 1)
    listed = position < page_count - layer * page_count // (2 * layers)
    source = jnp.where(listed, keep_list // blk_dev, -2)
    owner = jnp.where(listed, page_slot // page_dev, -2)
    crossing = (source // 2) != (owner // 2)
    pools = [jnp.sum(crossing & (source == s), dtype=jnp.int32) for s in range(4)]
    largest = functools.reduce(jnp.maximum, pools).reshape(1)
    size = lax.axis_size("groups")
    told = largest
    for step in range(1, size):
        passed = lax.ppermute(told, "groups", [(i, (i + step) % size) for i in range(size)])
        largest = jnp.maximum(largest, passed)
    sizes = range(2, cap // 2 + 1)
    shared = jnp.clip(2 * cap - largest[0], 0, sizes[-1])
    fits = jnp.maximum(shared - 1, 0)
    shared = jnp.where(fits > 0, shared, 0)
    alone = cap - shared

    pair = source * 4 + owner
    before = (layer[:, :, None, None] > layer[None, None]) | (
        (layer[:, :, None, None] == layer[None, None])
        & (position[:, :, None, None] > position[None, None])
    )
    rank = jnp.sum((pair[:, :, None, None] == pair[None, None]) & before, axis=(2, 3), dtype=jnp.int32)
    to_far = crossing & ((owner == 0) | (owner == 3))
    spill = rank - alone
    lone = rank < alone
    in_region = jnp.where(
        crossing,
        jnp.where(lone, shared + rank, jnp.where(to_far, shared - 1 - spill, spill)),
        rank,
    )
    sent = jnp.where(
        crossing,
        in_region + jnp.where(to_far & lone, alone, 0),
        in_region + jnp.where(source == owner, 3 * cap, 2 * cap),
    )
    got = in_region + jnp.where(
        crossing, (source % 2) * cap, jnp.where(source == owner, 3 * cap, 2 * cap)
    )
    spots = jnp.arange(4 * cap, dtype=jnp.int32)[:, None, None]
    pack_table = jnp.sum(
        jnp.where(
            (source == me) & (sent == spots), layer * blk_dev + keep_list % blk_dev, 0
        ),
        axis=(1, 2),
        dtype=jnp.int32,
    )
    pages = jnp.arange(layers * page_dev, dtype=jnp.int32)[:, None, None]
    place_table = 4 * cap + jnp.sum(
        jnp.where(
            (owner == me) & (layer * page_dev + page_slot % page_dev == pages), got - 4 * cap, 0
        ),
        axis=(1, 2),
        dtype=jnp.int32,
    )

    pack_table, place_table = lax.optimization_barrier((pack_table, place_table))
    packed = pl.pallas_call(
        pack_kernel,
        out_shape=pltpu.VMEM((4 * cap,) + page, kv_cache.dtype),
        in_specs=[SMEM, HBM],
        out_specs=VMEM,
        scratch_shapes=[dma((4 * cap,))],
        compiler_params=pltpu.CompilerParams(vmem_limit_bytes=PACK_GRANT),
    )(pack_table, kv_cache.reshape((layers * blk_dev,) + page))

    def deliver(shared, collective, packed, place_table):
        slots, bounds = exchange(cap, shared, collective, packed, heads, width)
        return pl.pallas_call(
            place_kernel,
            out_shape=(
                jax.ShapeDtypeStruct((layers * page_dev,) + page, kv_cache.dtype),
                jax.ShapeDtypeStruct((layers * page_dev, heads, 2, width), kv_cache.dtype),
            ),
            in_specs=[SMEM, VMEM, VMEM],
            out_specs=(HBM, VMEM),
            scratch_shapes=[dma((layers * page_dev,))],
            compiler_params=pltpu.CompilerParams(vmem_limit_bytes=GRANT),
        )(place_table, slots, bounds)

    paged, page_bounds = lax.switch(
        fits,
        [functools.partial(deliver, s, k) for k, s in enumerate([0, *sizes])],
        packed,
        place_table,
    )
    return (
        paged.reshape((layers, page_dev) + page),
        page_bounds.reshape(layers, page_dev, heads, 2, width),
    )


def on_device(kv_cache, keep_list, page_slot):
    body = line_of_four if lax.axis_size("seq") == 4 else any_line
    return body(kv_cache, keep_list, page_slot)


def solution(mesh):
    in_specs = (
        P(None, ("groups", "seq"), "head", "rep", None),
        P("groups", None),
        P("groups", None),
    )
    out_specs = (
        P(None, ("groups", "seq"), "head", "rep", None),
        P(None, ("groups", "seq"), "head", None, None),
    )
    return jax.shard_map(
        on_device, mesh=mesh, in_specs=in_specs, out_specs=out_specs, check_vma=False
    )
```

```python
import functools

import jax
import jax.numpy as jnp
from jax import lax
from jax.experimental import pallas as pl
from jax.experimental.pallas import tpu as pltpu
from jax.sharding import PartitionSpec as P

MESH = pl.DeviceIdType.MESH
HBM = pl.BlockSpec(memory_space=pltpu.HBM)
SMEM = pl.BlockSpec(memory_space=pltpu.SMEM)
GRANT = 8 << 20
PACK_GRANT = 54 << 20
VMEM = pl.BlockSpec(memory_space=pltpu.VMEM)


def combined_all(part, axis, combine):
    gathered = jax.tree.map(lambda a: lax.all_gather(a, axis), part)

    def take(source):
        return jax.tree.map(lambda a: lax.dynamic_index_in_dim(a, source, 0, False), gathered)

    return lax.fori_loop(
        1, lax.axis_size(axis), lambda source, state: combine(state, take(source)), take(0)
    )


def pack_slots(block_rows, sent_here, destination, local_block, slot_width):
    blk_dev = block_rows.shape[1]
    slot_hot = (
        destination[:, :, None] == jnp.arange(slot_width, dtype=jnp.int32)[None, None, :]
    ) & sent_here[:, :, None]
    block_hot = local_block[:, :, None] == jnp.arange(blk_dev, dtype=jnp.int32)[None, None, :]
    select = jnp.einsum(
        "ljw,ljb->lwb", slot_hot.astype(jnp.float32), block_hot.astype(jnp.float32)
    ).astype(jnp.bfloat16)
    return jnp.einsum(
        "lwb,lbr->lwr", select, block_rows, preferred_element_type=jnp.float32
    ).astype(jnp.bfloat16)


def place_index(takers, in_page, incoming, page_dev):
    page_hot = (
        in_page[:, :, None] == jnp.arange(page_dev, dtype=jnp.int32)[None, None, :]
    ) & takers[:, :, None]
    return jnp.sum(jnp.where(page_hot, incoming[:, :, None] + 1, 0), axis=1) - 1


def place_pages(target, shard_part):
    width = shard_part.shape[1]
    one_hot = (target[:, :, None] == jnp.arange(width, dtype=jnp.int32)[None, None, :]).astype(
        jnp.bfloat16
    )
    return jnp.einsum("lpn,lnr->lpr", one_hot, shard_part, preferred_element_type=jnp.float32)


def extend(first, second):
    return (jnp.maximum(first[0], second[0]), jnp.minimum(first[1], second[1]))


def any_line(kv_cache, keep_list, page_slot):
    layer_count, page_count = keep_list.shape
    blk_dev = kv_cache.shape[1]
    seq_count = lax.axis_size("seq")
    page_dev = page_count // seq_count
    capacity = (page_dev - 2) // seq_count + 2
    seq_index = lax.axis_index("seq")
    block_rows = kv_cache.reshape(layer_count, blk_dev, -1)
    position = jnp.arange(page_count, dtype=jnp.int32)
    counts = jnp.array(
        [page_count - layer * page_count // (2 * layer_count) for layer in range(layer_count)],
        jnp.int32,
    )
    listed = position[None, :] < counts[:, None]
    source = keep_list // blk_dev
    local_block = keep_list % blk_dev
    owner_index = page_slot // page_dev
    in_page = page_slot % page_dev
    earlier = (position[None, None, :] < position[None, :, None]) & listed[:, None, :]
    same_source = source[:, :, None] == source[:, None, :]
    sent_here = listed & (source == seq_index)
    takers = listed & (owner_index == seq_index)
    same_owner = owner_index[:, :, None] == owner_index[:, None, :]
    slot_rank = jnp.sum(earlier & same_source & same_owner, axis=2)
    packed = pack_slots(
        block_rows, sent_here, owner_index * capacity + slot_rank, local_block, seq_count * capacity
    )
    received = lax.all_to_all(packed, "seq", split_axis=1, concat_axis=1, tiled=True)
    target = place_index(takers, in_page, source * capacity + slot_rank, page_dev)
    gathered = place_pages(target, received)
    paged_cache = gathered.astype(jnp.bfloat16).reshape(
        (layer_count, page_dev) + kv_cache.shape[2:]
    )
    head_width = kv_cache.shape[-1] // 2
    key_part = paged_cache[..., :head_width]
    key_high = jnp.max(key_part, axis=3)
    key_low = jnp.min(key_part, axis=3)
    upper_bound, lower_bound = combined_all((key_high, key_low), "rep", extend)
    page_bounds = jnp.stack([upper_bound, lower_bound], axis=3)
    return (paged_cache, page_bounds)


def pack_kernel(table, blocks, packed, read_sem):
    count = packed.shape[0]

    def read(k):
        return pltpu.make_async_copy(blocks.at[table[k]], packed.at[k], read_sem.at[k])

    @pl.loop(0, count, unroll=4)
    def _(k):
        @pl.when(table[k] >= 0)
        def _():
            read(k).start()

    @pl.loop(0, count, unroll=4)
    def _(k):
        @pl.when(table[k] >= 0)
        def _():
            read(k).wait()


def place_kernel(table, slots, bounds, pages, page_bounds, write_sem):
    count, heads = page_bounds.shape[0], page_bounds.shape[1]

    def write(k):
        return pltpu.make_async_copy(slots.at[table[k]], pages.at[k], write_sem.at[k])

    @pl.loop(0, count)
    def _(k):
        write(k).start()

    @pl.loop(0, count)
    def _(k):
        both = bounds[table[k]]
        page_bounds[k] = jnp.stack([both[:heads], both[heads:]], axis=1).astype(page_bounds.dtype)

    @pl.loop(0, count)
    def _(k):
        write(k).wait()


def exchange_kernel(
    cap, shared, packed, held, bounds,
    mine, theirs, send_sem, recv_sem, relay_sem, rep_send, rep_recv,
):
    me = lax.axis_index("seq")
    half, lane = me // 2, me % 2
    partner = me + 1 - 2 * lane
    near, far = 2 - half, 3 - 3 * half
    inner = half + lane == 1
    other = 1 - lax.axis_index("rep")
    alone = cap - shared
    heads, width = held.shape[1], mine.shape[2]

    barrier = pltpu.get_barrier_semaphore()
    for step in range(1, 4):
        pl.semaphore_signal(
            barrier, inc=1, device_id={"seq": (me + step) % 4}, device_id_type=MESH
        )
    pl.semaphore_signal(barrier, inc=1, device_id={"rep": other}, device_id_type=MESH)
    pl.semaphore_wait(barrier, 4)

    def remote(source, place, target, sem):
        return pltpu.make_async_remote_copy(
            src_ref=source,
            dst_ref=held.at[place],
            send_sem=sem,
            recv_sem=recv_sem.at[place],
            device_id={"seq": target},
            device_id_type=MESH,
        )

    def to_near(q):
        return remote(packed.at[q], lane * cap + q, near, send_sem.at[q])

    def to_far(q):
        return remote(packed.at[q + alone], lane * cap + q, far, send_sem.at[q + alone])

    def to_partner(q):
        return remote(packed.at[2 * cap + q], 2 * cap + q, partner, send_sem.at[2 * cap + q])

    def relay(place, sem):
        return remote(held.at[place], place, partner, relay_sem.at[sem])

    def landed(place):
        pltpu.make_async_copy(held.at[place], held.at[place], recv_sem.at[place]).wait()

    def finish(place):
        extremes(place, held[place, :, :, :width])

    def extremes(place, keys):
        keys = keys.astype(jnp.float32)
        mine[place, :heads] = jnp.max(keys, axis=1)
        mine[place, heads:] = jnp.min(keys, axis=1)

    def swap(start, count, k):
        return pltpu.make_async_remote_copy(
            src_ref=mine.at[pl.ds(start, count)],
            dst_ref=theirs.at[pl.ds(start, count)],
            send_sem=rep_send.at[k],
            recv_sem=rep_recv.at[k],
            device_id={"rep": other},
            device_id_type=MESH,
        )

    def join(start, count):
        @pl.loop(0, count)
        def _(q):
            a, b = mine[start + q], theirs[start + q]
            bounds[start + q, :heads] = jnp.maximum(a[:heads], b[:heads])
            bounds[start + q, heads:] = jnp.minimum(a[heads:], b[heads:])

    @pl.when(jnp.logical_not(inner))
    def _():
        @pl.loop(0, cap)
        def _(q):
            to_partner(q).start()

    @pl.loop(0, shared)
    def _(q):
        to_near(q).start()

    @pl.loop(shared, cap)
    def _(q):
        to_far(q).start()
        to_near(q).start()

    @pl.when(inner)
    def _():
        @pl.loop(0, cap)
        def _(q):
            to_partner(q).start()

    empty = 4 * cap
    held[empty] = jnp.zeros(held.shape[1:], held.dtype)
    bounds[empty] = jnp.zeros(bounds.shape[1:], bounds.dtype)

    @pl.loop(0, cap)
    def _(q):
        block = packed[3 * cap + q]
        held[3 * cap + q] = block
        extremes(3 * cap + q, block[:, :, :width])

    first, second = half * cap, (1 - half) * cap

    if shared:
        @pl.when(inner)
        def _():
            @pl.loop(0, shared)
            def _(q):
                landed(first + q)
                relay(first + q, q).start()

            @pl.loop(0, shared)
            def _(q):
                landed(second + q)
                relay(second + q, shared + q).start()

    @pl.loop(0, cap)
    def _(q):
        landed(2 * cap + q)
        finish(2 * cap + q)

    swap(2 * cap, 2 * cap, 0).start()

    def collect(start):
        if shared:
            @pl.when(jnp.logical_not(inner))
            def _():
                @pl.loop(0, shared)
                def _(q):
                    landed(start + q)

            @pl.loop(0, shared)
            def _(q):
                finish(start + q)

        @pl.loop(shared, cap)
        def _(q):
            landed(start + q)
            finish(start + q)

    collect(first)
    swap(2 * cap, 2 * cap, 0).wait()
    join(2 * cap, 2 * cap)
    swap(first, cap, 1).start()
    collect(second)

    swap(first, cap, 1).wait()
    join(first, cap)
    swap(second, cap, 2).start()

    @pl.loop(0, 2 * cap - shared)
    def _(q):
        to_near(q).wait_send()

    @pl.loop(0, cap)
    def _(q):
        to_partner(q).wait_send()

    if shared:
        @pl.when(inner)
        def _():
            @pl.loop(0, shared)
            def _(q):
                relay(first + q, q).wait_send()
                relay(second + q, shared + q).wait_send()

    swap(second, cap, 2).wait()
    join(second, cap)


def exchange(cap, shared, collective, packed, heads, width):
    page = packed.shape[1:]
    count = 4 * cap + 1
    dma = pltpu.SemaphoreType.DMA
    return pl.pallas_call(
        functools.partial(exchange_kernel, cap, shared),
        out_shape=(
            pltpu.VMEM((count,) + page, packed.dtype),
            pltpu.VMEM((count, 2 * heads, width), jnp.float32),
        ),
        in_specs=[VMEM],
        out_specs=(VMEM, VMEM),
        scratch_shapes=[
            pltpu.VMEM((4 * cap, 2 * heads, width), jnp.float32),
            pltpu.VMEM((4 * cap, 2 * heads, width), jnp.float32),
            dma((3 * cap,)),
            dma((3 * cap,)),
            dma((max(2 * shared, 1),)),
            dma((3,)),
            dma((3,)),
        ],
        compiler_params=pltpu.CompilerParams(
            collective_id=collective, has_side_effects=True, vmem_limit_bytes=GRANT
        ),
    )(packed)


def line_of_four(kv_cache, keep_list, page_slot):
    layers, page_count = keep_list.shape
    blk_dev = kv_cache.shape[1]
    page = kv_cache.shape[2:]
    heads, width = page[0], page[-1] // 2
    page_dev = page_count // 4
    cap = layers * ((page_dev - 2) // 4 + 2)
    dma = pltpu.SemaphoreType.DMA
    me = lax.axis_index("seq")

    shape = (layers, page_count)
    layer = lax.broadcasted_iota(jnp.int32, shape, 0)
    position = lax.broadcasted_iota(jnp.int32, shape, 1)
    listed = position < page_count - layer * page_count // (2 * layers)
    source = jnp.where(listed, keep_list // blk_dev, -2)
    owner = jnp.where(listed, page_slot // page_dev, -2)
    crossing = (source // 2) != (owner // 2)
    sources = lax.broadcasted_iota(jnp.int32, (4,) + shape, 0)
    pools = jnp.sum(crossing & (source == sources), axis=(1, 2), dtype=jnp.int32)
    size = lax.axis_size("groups")
    told = pools
    for step in range(1, size):
        passed = lax.ppermute(told, "groups", [(i, (i + step) % size) for i in range(size)])
        pools = jnp.maximum(pools, passed)
    sizes = range(2, cap // 2 + 1)
    shared = jnp.clip(2 * cap - jnp.max(pools), 0, sizes[-1])
    fits = jnp.maximum(shared - 1, 0)
    shared = jnp.where(fits > 0, shared, 0)
    alone = cap - shared

    pair = source * 4 + owner
    before = (layer[:, :, None, None] > layer[None, None]) | (
        (layer[:, :, None, None] == layer[None, None])
        & (position[:, :, None, None] > position[None, None])
    )
    rank = jnp.sum((pair[:, :, None, None] == pair[None, None]) & before, axis=(2, 3), dtype=jnp.int32)
    to_far = crossing & ((owner == 0) | (owner == 3))
    spill = rank - alone
    lone = rank < alone
    in_region = jnp.where(
        crossing,
        jnp.where(lone, shared + rank, jnp.where(to_far, shared - 1 - spill, spill)),
        rank,
    )
    sent = jnp.where(
        crossing,
        in_region + jnp.where(to_far & lone, alone, 0),
        in_region + jnp.where(source == owner, 3 * cap, 2 * cap),
    )
    got = in_region + jnp.where(
        crossing, (source % 2) * cap, jnp.where(source == owner, 3 * cap, 2 * cap)
    )
    spots = jnp.arange(4 * cap, dtype=jnp.int32)[:, None, None]
    pack_table = jnp.sum(
        jnp.where(
            (source == me) & (sent == spots), layer * blk_dev + keep_list % blk_dev + 1, 0
        ),
        axis=(1, 2),
        dtype=jnp.int32,
    ) - 1
    pages = jnp.arange(layers * page_dev, dtype=jnp.int32)[:, None, None]
    place_table = 4 * cap + jnp.sum(
        jnp.where(
            (owner == me) & (layer * page_dev + page_slot % page_dev == pages), got - 4 * cap, 0
        ),
        axis=(1, 2),
        dtype=jnp.int32,
    )

    pack_table, place_table = lax.optimization_barrier((pack_table, place_table))
    packed = pl.pallas_call(
        pack_kernel,
        out_shape=pltpu.VMEM((4 * cap,) + page, kv_cache.dtype),
        in_specs=[SMEM, HBM],
        out_specs=VMEM,
        scratch_shapes=[dma((4 * cap,))],
        compiler_params=pltpu.CompilerParams(vmem_limit_bytes=PACK_GRANT),
    )(pack_table, kv_cache.reshape((layers * blk_dev,) + page))

    def deliver(shared, collective, packed, place_table):
        slots, bounds = exchange(cap, shared, collective, packed, heads, width)
        return pl.pallas_call(
            place_kernel,
            out_shape=(
                jax.ShapeDtypeStruct((layers * page_dev,) + page, kv_cache.dtype),
                jax.ShapeDtypeStruct((layers * page_dev, heads, 2, width), kv_cache.dtype),
            ),
            in_specs=[SMEM, VMEM, VMEM],
            out_specs=(HBM, VMEM),
            scratch_shapes=[dma((layers * page_dev,))],
            compiler_params=pltpu.CompilerParams(vmem_limit_bytes=GRANT),
        )(place_table, slots, bounds)

    paged, page_bounds = lax.switch(
        fits,
        [functools.partial(deliver, s, k) for k, s in enumerate([0, *sizes])],
        packed,
        place_table,
    )
    return (
        paged.reshape((layers, page_dev) + page),
        page_bounds.reshape(layers, page_dev, heads, 2, width),
    )


def on_device(kv_cache, keep_list, page_slot):
    body = line_of_four if lax.axis_size("seq") == 4 else any_line
    return body(kv_cache, keep_list, page_slot)


def solution(mesh):
    in_specs = (
        P(None, ("groups", "seq"), "head", "rep", None),
        P("groups", None),
        P("groups", None),
    )
    out_specs = (
        P(None, ("groups", "seq"), "head", "rep", None),
        P(None, ("groups", "seq"), "head", None, None),
    )
    return jax.shard_map(
        on_device, mesh=mesh, in_specs=in_specs, out_specs=out_specs, check_vma=False
    )
```

```python
import functools

import jax
import jax.numpy as jnp
from jax import lax
from jax.experimental import pallas as pl
from jax.experimental.pallas import tpu as pltpu
from jax.sharding import PartitionSpec as P

MESH = pl.DeviceIdType.MESH
HBM = pl.BlockSpec(memory_space=pltpu.HBM)
SMEM = pl.BlockSpec(memory_space=pltpu.SMEM)
GRANT = 8 << 20
PACK_GRANT = 54 << 20
VMEM = pl.BlockSpec(memory_space=pltpu.VMEM)


def combined_all(part, axis, combine):
    gathered = jax.tree.map(lambda a: lax.all_gather(a, axis), part)

    def take(source):
        return jax.tree.map(lambda a: lax.dynamic_index_in_dim(a, source, 0, False), gathered)

    return lax.fori_loop(
        1, lax.axis_size(axis), lambda source, state: combine(state, take(source)), take(0)
    )


def pack_slots(block_rows, sent_here, destination, local_block, slot_width):
    blk_dev = block_rows.shape[1]
    slot_hot = (
        destination[:, :, None] == jnp.arange(slot_width, dtype=jnp.int32)[None, None, :]
    ) & sent_here[:, :, None]
    block_hot = local_block[:, :, None] == jnp.arange(blk_dev, dtype=jnp.int32)[None, None, :]
    select = jnp.einsum(
        "ljw,ljb->lwb", slot_hot.astype(jnp.float32), block_hot.astype(jnp.float32)
    ).astype(jnp.bfloat16)
    return jnp.einsum(
        "lwb,lbr->lwr", select, block_rows, preferred_element_type=jnp.float32
    ).astype(jnp.bfloat16)


def place_index(takers, in_page, incoming, page_dev):
    page_hot = (
        in_page[:, :, None] == jnp.arange(page_dev, dtype=jnp.int32)[None, None, :]
    ) & takers[:, :, None]
    return jnp.sum(jnp.where(page_hot, incoming[:, :, None] + 1, 0), axis=1) - 1


def place_pages(target, shard_part):
    width = shard_part.shape[1]
    one_hot = (target[:, :, None] == jnp.arange(width, dtype=jnp.int32)[None, None, :]).astype(
        jnp.bfloat16
    )
    return jnp.einsum("lpn,lnr->lpr", one_hot, shard_part, preferred_element_type=jnp.float32)


def extend(first, second):
    return (jnp.maximum(first[0], second[0]), jnp.minimum(first[1], second[1]))


def any_line(kv_cache, keep_list, page_slot):
    layer_count, page_count = keep_list.shape
    blk_dev = kv_cache.shape[1]
    seq_count = lax.axis_size("seq")
    page_dev = page_count // seq_count
    capacity = (page_dev - 2) // seq_count + 2
    seq_index = lax.axis_index("seq")
    block_rows = kv_cache.reshape(layer_count, blk_dev, -1)
    position = jnp.arange(page_count, dtype=jnp.int32)
    counts = jnp.array(
        [page_count - layer * page_count // (2 * layer_count) for layer in range(layer_count)],
        jnp.int32,
    )
    listed = position[None, :] < counts[:, None]
    source = keep_list // blk_dev
    local_block = keep_list % blk_dev
    owner_index = page_slot // page_dev
    in_page = page_slot % page_dev
    earlier = (position[None, None, :] < position[None, :, None]) & listed[:, None, :]
    same_source = source[:, :, None] == source[:, None, :]
    sent_here = listed & (source == seq_index)
    takers = listed & (owner_index == seq_index)
    same_owner = owner_index[:, :, None] == owner_index[:, None, :]
    slot_rank = jnp.sum(earlier & same_source & same_owner, axis=2)
    packed = pack_slots(
        block_rows, sent_here, owner_index * capacity + slot_rank, local_block, seq_count * capacity
    )
    received = lax.all_to_all(packed, "seq", split_axis=1, concat_axis=1, tiled=True)
    target = place_index(takers, in_page, source * capacity + slot_rank, page_dev)
    gathered = place_pages(target, received)
    paged_cache = gathered.astype(jnp.bfloat16).reshape(
        (layer_count, page_dev) + kv_cache.shape[2:]
    )
    head_width = kv_cache.shape[-1] // 2
    key_part = paged_cache[..., :head_width]
    key_high = jnp.max(key_part, axis=3)
    key_low = jnp.min(key_part, axis=3)
    upper_bound, lower_bound = combined_all((key_high, key_low), "rep", extend)
    page_bounds = jnp.stack([upper_bound, lower_bound], axis=3)
    return (paged_cache, page_bounds)


def pack_kernel(table, blocks, packed, read_sem):
    count = packed.shape[0]

    def read(k):
        return pltpu.make_async_copy(blocks.at[table[k]], packed.at[k], read_sem.at[k])

    @pl.loop(0, count, unroll=4)
    def _(k):
        @pl.when(table[k] >= 0)
        def _():
            read(k).start()

    @pl.loop(0, count, unroll=4)
    def _(k):
        @pl.when(table[k] >= 0)
        def _():
            read(k).wait()


def place_kernel(table, slots, bounds, pages, page_bounds, write_sem):
    count, heads = page_bounds.shape[0], page_bounds.shape[1]

    def write(k):
        return pltpu.make_async_copy(slots.at[table[k]], pages.at[k], write_sem.at[k])

    @pl.loop(0, count)
    def _(k):
        write(k).start()

    @pl.loop(0, count)
    def _(k):
        both = bounds[table[k]]
        page_bounds[k] = jnp.stack([both[:heads], both[heads:]], axis=1).astype(page_bounds.dtype)

    @pl.loop(0, count)
    def _(k):
        write(k).wait()


def exchange_kernel(
    cap, shared, extra, packed, choice, held, bounds,
    mine, theirs, incoming, merged, send_sem, recv_sem, relay_sem, extra_send, extra_recv,
    rep_send, rep_recv,
):
    me = lax.axis_index("seq")
    half, lane = me // 2, me % 2
    partner = me + 1 - 2 * lane
    near, far = 2 - half, 3 - 3 * half
    inner = half + lane == 1
    other = 1 - lax.axis_index("rep")
    alone = cap - shared
    heads, width = held.shape[1], mine.shape[2]

    barrier = pltpu.get_barrier_semaphore()
    for step in range(1, 4):
        pl.semaphore_signal(
            barrier, inc=1, device_id={"seq": (me + step) % 4}, device_id_type=MESH
        )
    pl.semaphore_signal(barrier, inc=1, device_id={"rep": other}, device_id_type=MESH)
    pl.semaphore_wait(barrier, 4)

    def remote(source, place, target, sem):
        return pltpu.make_async_remote_copy(
            src_ref=source,
            dst_ref=held.at[place],
            send_sem=sem,
            recv_sem=recv_sem.at[place],
            device_id={"seq": target},
            device_id_type=MESH,
        )

    def to_near(q):
        return remote(packed.at[q], lane * cap + q, near, send_sem.at[q])

    def to_far(q):
        return remote(packed.at[q + alone], lane * cap + q, far, send_sem.at[q + alone])

    def to_partner(q):
        return remote(packed.at[2 * cap + q], 2 * cap + q, partner, send_sem.at[2 * cap + q])

    def relay(place, sem):
        return remote(held.at[place], place, partner, relay_sem.at[sem])

    def landed(place):
        pltpu.make_async_copy(held.at[place], held.at[place], recv_sem.at[place]).wait()

    def finish(place):
        extremes(place, held[place, :, :, :width])

    def extremes(place, keys):
        keys = keys.astype(jnp.float32)
        mine[place, :heads] = jnp.max(keys, axis=1)
        mine[place, heads:] = jnp.min(keys, axis=1)

    def swap(start, count, k):
        return pltpu.make_async_remote_copy(
            src_ref=mine.at[pl.ds(start, count)],
            dst_ref=theirs.at[pl.ds(start, count)],
            send_sem=rep_send.at[k],
            recv_sem=rep_recv.at[k],
            device_id={"rep": other},
            device_id_type=MESH,
        )

    def join(start, count):
        @pl.loop(0, count)
        def _(q):
            a, b = mine[start + q], theirs[start + q]
            bounds[start + q, :heads] = jnp.maximum(a[:heads], b[:heads])
            bounds[start + q, heads:] = jnp.minimum(a[heads:], b[heads:])

    def to_inner(v):
        return pltpu.make_async_remote_copy(
            src_ref=packed.at[4 * cap + v],
            dst_ref=incoming.at[v],
            send_sem=extra_send.at[v],
            recv_sem=extra_recv.at[v],
            device_id={"seq": partner},
            device_id_type=MESH,
        )

    def across(v):
        return remote(merged.at[v], 4 * cap + v, near, extra_send.at[v])

    @pl.when(jnp.logical_not(inner))
    def _():
        if extra:
            @pl.loop(0, extra)
            def _(v):
                to_inner(v).start()

        @pl.loop(0, cap)
        def _(q):
            to_partner(q).start()

    @pl.loop(0, shared)
    def _(q):
        to_near(q).start()

    @pl.loop(shared, cap)
    def _(q):
        to_far(q).start()
        to_near(q).start()

    @pl.when(inner)
    def _():
        @pl.loop(0, cap)
        def _(q):
            to_partner(q).start()

    if extra:
        @pl.when(inner)
        def _():
            @pl.loop(0, extra)
            def _(v):
                to_inner(v).wait_recv()
                merged[v] = jnp.where(
                    choice[v] > 0,
                    packed[4 * cap + v].astype(jnp.float32),
                    incoming[v].astype(jnp.float32),
                ).astype(merged.dtype)

    empty = held.shape[0] - 1
    held[empty] = jnp.zeros(held.shape[1:], held.dtype)
    bounds[empty] = jnp.zeros(bounds.shape[1:], bounds.dtype)

    @pl.loop(0, cap)
    def _(q):
        block = packed[3 * cap + q]
        held[3 * cap + q] = block
        extremes(3 * cap + q, block[:, :, :width])

    first, second = half * cap, (1 - half) * cap

    if extra:
        @pl.when(inner)
        def _():
            @pl.loop(0, extra)
            def _(v):
                across(v).start()


    if shared:
        @pl.when(inner)
        def _():
            @pl.loop(0, shared)
            def _(q):
                landed(first + q)
                relay(first + q, q).start()

            @pl.loop(0, shared)
            def _(q):
                landed(second + q)
                relay(second + q, shared + q).start()

    @pl.loop(0, cap)
    def _(q):
        landed(2 * cap + q)
        finish(2 * cap + q)

    swap(2 * cap, 2 * cap, 0).start()

    def collect(start):
        if shared:
            @pl.when(jnp.logical_not(inner))
            def _():
                @pl.loop(0, shared)
                def _(q):
                    landed(start + q)

            @pl.loop(0, shared)
            def _(q):
                finish(start + q)

        @pl.loop(shared, cap)
        def _(q):
            landed(start + q)
            finish(start + q)

    collect(first)
    swap(2 * cap, 2 * cap, 0).wait()
    join(2 * cap, 2 * cap)
    swap(first, cap, 1).start()
    collect(second)

    swap(first, cap, 1).wait()
    join(first, cap)
    swap(second, cap, 2).start()

    if extra:
        @pl.when(inner)
        def _():
            @pl.loop(0, extra)
            def _(v):
                landed(4 * cap + v)
                finish(4 * cap + v)

            swap(4 * cap, extra, 3).start()

    @pl.loop(0, 2 * cap - shared)
    def _(q):
        to_near(q).wait_send()

    @pl.loop(0, cap)
    def _(q):
        to_partner(q).wait_send()

    if shared:
        @pl.when(inner)
        def _():
            @pl.loop(0, shared)
            def _(q):
                relay(first + q, q).wait_send()
                relay(second + q, shared + q).wait_send()

    swap(second, cap, 2).wait()
    join(second, cap)

    if extra:
        @pl.loop(0, extra)
        def _(v):
            to_inner(v).wait_send()

        @pl.when(inner)
        def _():
            swap(4 * cap, extra, 3).wait()
            join(4 * cap, extra)


def exchange(cap, shared, extra, collective, packed, choice, heads, width):
    page = packed.shape[1:]
    count = packed.shape[0] + 1
    dma = pltpu.SemaphoreType.DMA
    return pl.pallas_call(
        functools.partial(exchange_kernel, cap, shared, extra),
        out_shape=(
            pltpu.VMEM((count,) + page, packed.dtype),
            pltpu.VMEM((count, 2 * heads, width), jnp.float32),
        ),
        in_specs=[VMEM, VMEM],
        out_specs=(VMEM, VMEM),
        scratch_shapes=[
            pltpu.VMEM((count, 2 * heads, width), jnp.float32),
            pltpu.VMEM((count, 2 * heads, width), jnp.float32),
            pltpu.VMEM((max(extra, 1),) + page, packed.dtype),
            pltpu.VMEM((max(extra, 1),) + page, packed.dtype),
            dma((3 * cap,)),
            dma((count,)),
            dma((max(2 * shared, 1),)),
            dma((max(extra, 1),)),
            dma((max(extra, 1),)),
            dma((4,)),
            dma((4,)),
        ],
        compiler_params=pltpu.CompilerParams(
            collective_id=collective, has_side_effects=True, vmem_limit_bytes=GRANT
        ),
    )(packed, choice)


def line_of_four(kv_cache, keep_list, page_slot):
    layers, page_count = keep_list.shape
    blk_dev = kv_cache.shape[1]
    page = kv_cache.shape[2:]
    heads, width = page[0], page[-1] // 2
    page_dev = page_count // 4
    cap = layers * ((page_dev - 2) // 4 + 2)
    dma = pltpu.SemaphoreType.DMA
    me = lax.axis_index("seq")

    shape = (layers, page_count)
    layer = lax.broadcasted_iota(jnp.int32, shape, 0)
    position = lax.broadcasted_iota(jnp.int32, shape, 1)
    listed = position < page_count - layer * page_count // (2 * layers)
    source = jnp.where(listed, keep_list // blk_dev, -2)
    owner = jnp.where(listed, page_slot // page_dev, -2)
    crossing = (source // 2) != (owner // 2)
    sources = lax.broadcasted_iota(jnp.int32, (4,) + shape, 0)
    pools = jnp.sum(crossing & (source == sources), axis=(1, 2), dtype=jnp.int32)
    apart, spare = 2 * cap // 5, cap // 2
    over = jnp.maximum(pools - (cap + apart), 0)
    size = lax.axis_size("groups")
    told = needs = jnp.sum(over.reshape(2, 2), axis=1)
    for step in range(1, size):
        passed = lax.ppermute(told, "groups", [(i, (i + step) % size) for i in range(size)])
        needs = jnp.maximum(needs, passed)
    need = jnp.max(needs)
    form = jnp.where(need > spare, 0, jnp.maximum(need, 1))
    shared = jnp.where(form > 0, cap - apart, 0)
    alone = cap - shared

    pair = source * 4 + owner
    before = (layer[:, :, None, None] > layer[None, None]) | (
        (layer[:, :, None, None] == layer[None, None])
        & (position[:, :, None, None] > position[None, None])
    )
    rank = jnp.sum((pair[:, :, None, None] == pair[None, None]) & before, axis=(2, 3), dtype=jnp.int32)
    to_far = crossing & ((owner == 0) | (owner == 3))
    to_near = crossing & ((owner == 1) | (owner == 2))
    same = (source == sources) & to_near
    close = jnp.sum(same, axis=(1, 2), dtype=jnp.int32)
    limit = jnp.where(form > 0, close - over, 2 * cap)
    late = rank - jnp.sum(
        jnp.where(source == sources, limit[:, None, None], 0), axis=0, dtype=jnp.int32
    )
    late = jnp.where(to_near, late, -1)
    behind = 4 * cap + jnp.where((source == 0) | (source == 3), form - 1 - late, late)
    spill = rank - alone
    lone = rank < alone
    in_region = jnp.where(
        crossing,
        jnp.where(lone, shared + rank, jnp.where(to_far, shared - 1 - spill, spill)),
        rank,
    )
    sent = jnp.where(
        crossing,
        in_region + jnp.where(to_far & lone, alone, 0),
        in_region + jnp.where(source == owner, 3 * cap, 2 * cap),
    )
    got = in_region + jnp.where(
        crossing, (source % 2) * cap, jnp.where(source == owner, 3 * cap, 2 * cap)
    )
    sent = jnp.where(late >= 0, behind, sent)
    got = jnp.where(late >= 0, behind, got)
    total = 4 * cap + spare
    mine_over = jnp.sum(
        jnp.where(jnp.arange(4, dtype=jnp.int32) == me, over, 0), dtype=jnp.int32
    )
    choice = jnp.where(
        lax.broadcasted_iota(jnp.int32, (spare, 1, page[-1]), 0) < mine_over, 1, 0
    ).astype(jnp.int32)
    spots = jnp.arange(total, dtype=jnp.int32)[:, None, None]
    pack_table = jnp.sum(
        jnp.where(
            (source == me) & (sent == spots), layer * blk_dev + keep_list % blk_dev + 1, 0
        ),
        axis=(1, 2),
        dtype=jnp.int32,
    ) - 1
    pages = jnp.arange(layers * page_dev, dtype=jnp.int32)[:, None, None]
    place_table = total + jnp.sum(
        jnp.where(
            (owner == me) & (layer * page_dev + page_slot % page_dev == pages), got - total, 0
        ),
        axis=(1, 2),
        dtype=jnp.int32,
    )

    pack_table, place_table, choice = lax.optimization_barrier((pack_table, place_table, choice))
    packed = pl.pallas_call(
        pack_kernel,
        out_shape=pltpu.VMEM((total,) + page, kv_cache.dtype),
        in_specs=[SMEM, HBM],
        out_specs=VMEM,
        scratch_shapes=[dma((total,))],
        compiler_params=pltpu.CompilerParams(vmem_limit_bytes=PACK_GRANT),
    )(pack_table, kv_cache.reshape((layers * blk_dev,) + page))

    def deliver(form, packed, choice, place_table):
        shared = cap - apart if form else 0
        slots, bounds = exchange(cap, shared, form, form, packed, choice, heads, width)
        return pl.pallas_call(
            place_kernel,
            out_shape=(
                jax.ShapeDtypeStruct((layers * page_dev,) + page, kv_cache.dtype),
                jax.ShapeDtypeStruct((layers * page_dev, heads, 2, width), kv_cache.dtype),
            ),
            in_specs=[SMEM, VMEM, VMEM],
            out_specs=(HBM, VMEM),
            scratch_shapes=[dma((layers * page_dev,))],
            compiler_params=pltpu.CompilerParams(vmem_limit_bytes=GRANT),
        )(place_table, slots, bounds)

    paged, page_bounds = lax.switch(
        form,
        [functools.partial(deliver, f) for f in range(spare + 1)],
        packed,
        choice,
        place_table,
    )
    return (
        paged.reshape((layers, page_dev) + page),
        page_bounds.reshape(layers, page_dev, heads, 2, width),
    )


def on_device(kv_cache, keep_list, page_slot):
    body = line_of_four if lax.axis_size("seq") == 4 else any_line
    return body(kv_cache, keep_list, page_slot)


def solution(mesh):
    in_specs = (
        P(None, ("groups", "seq"), "head", "rep", None),
        P("groups", None),
        P("groups", None),
    )
    out_specs = (
        P(None, ("groups", "seq"), "head", "rep", None),
        P(None, ("groups", "seq"), "head", None, None),
    )
    return jax.shard_map(
        on_device, mesh=mesh, in_specs=in_specs, out_specs=out_specs, check_vma=False
    )
```
